32 devices in a mesh: lon: 8 (over y, x, core), lev: 4 (over z).
Axes of the slice: x: 2, y: 2, z: 4, core: 2. Of those that a mesh axis runs over, the one named last changes fastest.
Arguments:
- field: float32 [72, 128, 128], P('lev', 'lon'), may hold values from -6 to 6
- ens: bfloat16 [80, 72, 128, 128], P(None, 'lev', 'lon'), may hold values from -2 to 2
- sdev: float32 [72, 128, 128], P('lev', 'lon'), may hold values from 0.5 to 2
- lon_taper: bfloat16 [17], replicated, may hold values from 0 to 0.079589844
- static_taper: bfloat16 [17], replicated, may hold values from 0 to 0.079589844
- loc_vert: bfloat16 [72, 72], P('lev'), may hold values from -0.75 to 0.75
- static_vert: bfloat16 [72, 72], P('lev'), may hold values from -0.75 to 0.75
- obs_block: int32 [8192], P('lon'), may hold values from -1 to 127, as said below
- obs_value: float32 [8192], P('lon'), may hold values from -6 to 6
- obs_rinv: float32 [8192], P('lon'), may hold values from 0.25 to 4
- obs_horiz: float32 [8192, 128], P('lon'), may hold values from -0.5 to 0.5
- obs_vert: float32 [8192, 72], P('lon', 'lev'), may hold values from -0.75 to 0.75
Outputs:
- increment: float32 [72, 128, 128], P('lev', 'lon')
- adjoint_field: float32 [72, 128, 128], P('lev', 'lon')
- obs_cost: float32 [], replicated
The draws below stay inside these ranges and needn't reach their ends.
Inputs may be any that keep to these rules, and one draw needn't show every extreme that they name: `obs_block`: each longitude sector's 1024 slots name only blocks within that sector's longitudes; live slots come first, in non-falling block order; at least half of a sector's slots are live, and some sector has all its slots live.
All inputs are finite; a program needn't handle non-finite values.
Results may differ from the reference program's by a relative error of at most 0.0041.
Values may be sent and summed in bfloat16 or wider, within the bound.
A program may use at most 128 MiB of HBM per device.

```python
import math
import jax
import jax.numpy as jnp
from jax import lax

ENS = 80
LEV = 72
LAT = 128
LON_DEV = 16
OBS_DEV = 1024
HALO = 8
NLON = 128
NOBS = 8192


def draw_obs_block(key, part):
    groups = NOBS // OBS_DEV
    per_group = LON_DEV // 8 * (LAT // 16)
    key_ids = jax.random.fold_in(key, 11)
    key_live = jax.random.fold_in(key, 23)
    local = jnp.sort(jax.random.randint(key_ids, (groups, OBS_DEV), 0, per_group), axis=1)
    counts = jax.random.randint(key_live, (groups, 1), OBS_DEV // 2, OBS_DEV + 1)
    counts = counts.at[0, 0].set(OBS_DEV)
    slots = jnp.arange(OBS_DEV)[None, :]
    base = jnp.arange(groups)[:, None] * per_group
    ids = jnp.where(slots < counts, local + base, -1)
    return ids.reshape(-1).astype(jnp.int32)


def steps_of(stream_key, dims, shards, least, high):
    level, own = 1.0, jax.random.fold_in(stream_key, 6)
    for position, blocks in shards:
        steps = jnp.exp(jax.random.uniform(jax.random.fold_in(own, position), (blocks,), jnp.float32, least / len(shards), high / len(shards)))
        level = level * jnp.repeat(steps, dims[position] // blocks).reshape([-1 if axis == position else 1 for axis in range(len(dims))])
    return level


def noise(rng, dims, spread, most, cuts=(), dtype=jnp.bfloat16):
    entries = spread * jax.random.normal(rng, dims, jnp.float32)
    if cuts:
        entries = entries * steps_of(rng, dims, cuts, -0.22, 0.18)
    return jnp.clip(entries, -most, most).astype(dtype)


def setup_inputs(seed: int = 0) -> dict:
    key_list = jax.random.split(jax.random.key(seed), 13)
    field = noise(key_list[0], (LEV, NLON, LAT), 1.0, 6.0, ((0, 4), (1, 8)), jnp.float32)
    ens = noise(key_list[1], (ENS, LEV, NLON, LAT), 0.3, 2.0, ((1, 4), (2, 8)))
    sdev = jnp.clip(jnp.exp(math.log(2.0) - 1.3862944 * jax.random.uniform(key_list[2], (LEV, NLON, LAT), jnp.float32) ** steps_of(key_list[2], (LEV, NLON, LAT), ((0, 4), (1, 8)), -0.2, 0.2)), 0.5, 2.0)
    lon_taper = jnp.clip(jax.random.uniform(key_list[3], (2 * HALO + 1,), jnp.float32, 0.0, 0.079589844), 0.0, 0.079589844).astype(jnp.bfloat16)
    static_taper = jnp.clip(jax.random.uniform(key_list[4], (2 * HALO + 1,), jnp.float32, 0.0, 0.079589844), 0.0, 0.079589844).astype(jnp.bfloat16)
    loc_vert = noise(key_list[5], (LEV, LEV), LEV ** -0.5, 0.75, ((0, 4),))
    static_vert = noise(key_list[6], (LEV, LEV), LEV ** -0.5, 0.75, ((0, 4),))
    obs_block = draw_obs_block(jax.random.fold_in(key_list[12], 71), 0)
    obs_value = noise(key_list[8], (NOBS,), 1.0, 6.0, ((0, 8),), jnp.float32)
    obs_rinv = jnp.clip(jnp.exp(math.log(4.0) - 2.7725887 * jax.random.uniform(key_list[9], (NOBS,), jnp.float32) ** steps_of(key_list[9], (NOBS,), ((0, 8),), -0.2, 0.2)), 0.25, 4.0)
    obs_horiz = noise(key_list[10], (NOBS, 128), 128 ** -0.5, 0.5, ((0, 8),), jnp.float32)
    obs_vert = noise(key_list[11], (NOBS, LEV), LEV ** -0.5, 0.75, ((0, 8), (1, 4)), jnp.float32)
    return dict(field=field, ens=ens, sdev=sdev, lon_taper=lon_taper, static_taper=static_taper, loc_vert=loc_vert, static_vert=static_vert, obs_block=obs_block, obs_value=obs_value, obs_rinv=obs_rinv, obs_horiz=obs_horiz, obs_vert=obs_vert)


ens_weight = 0.8
static_weight = 0.5


def localize(zfield, taper, vmatrix):
    width = taper.shape[0]
    half = width // 2
    total = jnp.zeros(zfield.shape, jnp.float32)
    for offset in range(width):
        total = total + taper[offset].astype(jnp.float32) * jnp.roll(zfield, half - offset, axis=1).astype(jnp.float32)
    smooth = total.astype(jnp.bfloat16)
    levels = smooth.shape[0]
    flat = smooth.reshape(levels, -1)
    return jnp.dot(vmatrix, flat, preferred_element_type=jnp.float32).reshape(zfield.shape)


def reference(field, ens, sdev, lon_taper, static_taper, loc_vert, static_vert, obs_block, obs_value, obs_rinv, obs_horiz, obs_vert):
    def member(total, pert):
        zpert = (pert.astype(jnp.float32) * field).astype(jnp.bfloat16)
        return total + pert.astype(jnp.float32) * localize(zpert, lon_taper, loc_vert), None

    ens_sum, _ = lax.scan(member, jnp.zeros(field.shape, jnp.float32), ens)
    spart = (sdev * field).astype(jnp.bfloat16)
    static_sum = localize(spart, static_taper, static_vert)
    increment = ens_weight * ens_sum + static_weight * sdev * static_sum
    nblk = (NLON // 8) * (LAT // 16)
    blocks = increment.reshape(LEV, NLON // 8, 8, LAT // 16, 16).transpose(0, 1, 3, 2, 4).reshape(LEV, nblk, 128)
    groups = NOBS // OBS_DEV
    ids = obs_block.reshape(groups, OBS_DEV)
    values = obs_value.reshape(groups, OBS_DEV)
    rinv = obs_rinv.reshape(groups, OBS_DEV)
    horiz = obs_horiz.reshape(groups, OBS_DEV, 128)
    vert = obs_vert.reshape(groups, OBS_DEV, LEV)

    def observe(carry, items):
        block_ids, value, weight, hpart, vpart = items
        live = block_ids >= 0
        safe = jnp.where(live, block_ids, 0).astype(jnp.int32)
        picked = jnp.take(blocks, safe, axis=1)
        hz = jnp.einsum('ljc,jc->lj', picked, hpart, precision=lax.Precision.HIGHEST)
        hx = jnp.einsum('jl,lj->j', vpart, hz, precision=lax.Precision.HIGHEST)
        miss = hx - value
        dep = jnp.where(live, weight * miss, 0.0)
        cost = 0.5 * jnp.sum(dep * miss)
        terms = (dep[:, None, None] * vpart[:, :, None]) * hpart[:, None, :]
        adj = jax.ops.segment_sum(terms, safe, num_segments=nblk)
        return (carry[0] + adj, carry[1] + cost), None

    init = (jnp.zeros((nblk, LEV, 128), jnp.float32), jnp.zeros((), jnp.float32))
    (adj_blocks, obs_cost), _ = lax.scan(observe, init, (ids, values, rinv, horiz, vert))
    adjoint_field = adj_blocks.transpose(1, 0, 2).reshape(LEV, NLON // 8, LAT // 16, 8, 16).transpose(0, 1, 3, 2, 4).reshape(LEV, NLON, LAT)
    return increment, adjoint_field, obs_cost
```

```python
import functools

import jax
import jax.numpy as jnp
from jax import lax
from jax.experimental import pallas as pl
from jax.experimental.pallas import tpu as pltpu
from jax.sharding import PartitionSpec as P

ens_weight = 0.8
static_weight = 0.5
MESH = pl.DeviceIdType.MESH
F32 = jnp.float32
BF16 = jnp.bfloat16


LINE = 8
GROUP = 16
LEAD = 0


def main_kernel(
    dims,
    ens,
    field_in,
    sdev_in,
    taper_in,
    static_taper_in,
    loc_in,
    svert_in,
    ids_in,
    value_in,
    rinv_in,
    horiz_in,
    vert_in,
    both,
    cost,
    field,
    sdev,
    taper,
    static_taper,
    loc,
    svert,
    ids,
    value,
    rinv,
    horiz,
    vert,
    ebuf,
    zbuf,
    hsend,
    fsend,
    fgroup,
    fbuf,
    spart,
    sband,
    sbuf,
    ssend,
    smooth,
    zs,
    lpad,
    spad,
    lg,
    spread,
    w,
    ws,
    pick,
    tband,
    acc,
    accb,
    rbuf,
    hturn,
    hcol,
    hrow,
    cells,
    vfold,
    vsend,
    vg,
    vx,
    part,
    parts,
    costs,
    own_sem,
    in_sem,
    ens_send,
    ens_recv,
    halo_send,
    halo_recv,
    small_send,
    small_recv,
    relay_send,
    back_send,
    back_recv,
    part_send,
    part_recv,
    cost_send,
    cost_recv,
):
    nlev, nlon, levs, cols, half, pairs = dims
    rows = levs * cols
    full = nlev * rows
    edge = nlev * levs * half
    wide = full + 2 * edge
    lead = min(LEAD, pairs)
    strip = levs * half
    hl = nlev // 2
    me = lax.axis_index("lev")
    lon = lax.axis_index("lon")
    right, left = lax.rem(lon + 1, nlon), lax.rem(lon + nlon - 1, nlon)
    peers = [lax.rem(me + off, nlev) for off in range(1, nlev)]
    sources = [lax.rem(me + nlev - off, nlev) for off in range(1, nlev)]
    side = me // hl
    gate = (me == hl - 1) | (me == hl)
    other_gate = hl - 1 + (1 - side)
    far_ranks = [(1 - side) * hl + q for q in range(hl)]
    near_ranks = [side * hl + lax.rem(me - side * hl + q, hl) for q in range(1, hl)]

    def slot(rank):
        return pl.ds(pl.multiple_of(rank * rows, 16), rows)

    own_copy = pltpu.make_async_copy(
        ens.at[pl.ds(me * 2 * pairs, 2 * pairs)], ebuf.at[:, slot(me)], own_sem
    )
    staged = (
        (field_in, field),
        (loc_in, loc),
        (svert_in, svert),
        (taper_in, taper),
        (static_taper_in, static_taper),
        (sdev_in, sdev),
        (ids_in, ids),
        (value_in, value),
        (rinv_in, rinv),
        (horiz_in, horiz),
        (vert_in, vert),
    )
    stage = [
        pltpu.make_async_copy(src, dst, in_sem.at[q]) for q, (src, dst) in enumerate(staged)
    ]
    for copy in stage:
        copy.start()
    own_copy.start()
    lons = [lax.rem(lon + off, nlon) for off in range(1, nlon)]

    barrier = pltpu.get_barrier_semaphore()
    for peer in peers:
        pl.semaphore_signal(barrier, inc=1, device_id={"lev": peer}, device_id_type=MESH)
    for peer in lons:
        pl.semaphore_signal(barrier, inc=1, device_id={"lon": peer}, device_id_type=MESH)
    width = loc.shape[1]
    stage[0].wait()
    fsend[...] = field[...].astype(BF16)
    fgroup[slot(me)] = fsend[...]
    for copy in stage[1:]:
        copy.wait()
    for matrix, padded in ((loc, lpad), (svert, spad)):
        padded[...] = jnp.zeros_like(padded)
        padded[:levs, :width] = matrix[...]
    spart[...] = (sdev[...] * field[...]).astype(BF16)
    slots = ids.shape[1]
    lats = field.shape[1]
    folds = slots // 128
    for q in range(folds):
        vfold[q * levs : (q + 1) * levs] = vert[:, q * 128 : (q + 1) * 128]
    vsend[...] = vfold[...].astype(BF16)
    pl.semaphore_wait(barrier, nlev + nlon - 2)

    def land(which, rank):
        dst = (lg, fgroup, zs, vg)[which]
        return dst.at[rank] if which in (0, 3) else dst.at[slot(rank)]

    def small(which, off, peer, rank):
        return pltpu.make_async_remote_copy(
            src_ref=(lpad, fsend, smooth, vsend)[which],
            dst_ref=land(which, rank),
            send_sem=small_send.at[which, off],
            recv_sem=small_recv.at[which, rank],
            device_id={"lev": peer},
            device_id_type=MESH,
        )

    def relay(which, q, k):
        return pltpu.make_async_remote_copy(
            src_ref=land(which, far_ranks[q]),
            dst_ref=land(which, far_ranks[q]),
            send_sem=relay_send.at[which, q * hl + k],
            recv_sem=small_recv.at[which, far_ranks[q]],
            device_id={"lev": near_ranks[k]},
            device_id_type=MESH,
        )

    def gather_start(which):
        for off, peer in enumerate(peers):

            @pl.when((peer // hl == side) | (peer == other_gate))
            def _(off=off, peer=peer):
                small(which, off, peer, me).start()

    def gather_far(which):
        for q, rank in enumerate(far_ranks):
            small(which, 0, peers[0], rank).wait_recv()

            @pl.when(gate)
            def _(q=q):
                for k in range(hl - 1):
                    relay(which, q, k).start()

    def gather_near(which):
        for rank in near_ranks:
            small(which, 0, peers[0], rank).wait_recv()

    def gather_drain(which):
        for off, peer in enumerate(peers):

            @pl.when((peer // hl == side) | (peer == other_gate))
            def _(off=off, peer=peer):
                small(which, off, peer, me).wait_send()

        @pl.when(gate)
        def _():
            for q in range(hl):
                for k in range(hl - 1):
                    relay(which, q, k).wait_send()

    def ens_copy(off, peer, rank, c):
        return pltpu.make_async_remote_copy(
            src_ref=ens.at[peer * 2 * pairs + c],
            dst_ref=ebuf.at[c, slot(rank)],
            send_sem=ens_send.at[off, c],
            recv_sem=ens_recv.at[rank, c],
            device_id={"lev": peer},
            device_id_type=MESH,
        )

    def halo_copy(side_to, c, h, rank=None):
        lane = pl.ds(h * 128, 128)
        base = full + side_to * edge
        if rank is None:
            src, dst = pl.ds(0, edge), pl.ds(base, edge)
        else:
            first = pl.multiple_of(rank * strip, 16)
            src, dst = pl.ds(first, strip), pl.ds(base + first, strip)
        return pltpu.make_async_remote_copy(
            src_ref=hsend.at[side_to, c, src, lane],
            dst_ref=zbuf.at[c, dst, lane],
            send_sem=halo_send.at[side_to, 2 * c + h],
            recv_sem=halo_recv.at[side_to, 2 * c + h],
            device_id={"lon": (right, left)[side_to]},
            device_id_type=MESH,
        )

    def static_halo(side_to):
        return pltpu.make_async_remote_copy(
            src_ref=ssend.at[side_to],
            dst_ref=sbuf.at[pl.ds(rows + side_to * strip, strip)],
            send_sem=halo_send.at[side_to, 2 * pairs],
            recv_sem=halo_recv.at[side_to, 2 * pairs],
            device_id={"lon": (right, left)[side_to]},
            device_id_type=MESH,
        )

    def back_copy(off, peer):
        return pltpu.make_async_remote_copy(
            src_ref=accb.at[slot(peer)],
            dst_ref=rbuf.at[off],
            send_sem=back_send.at[off],
            recv_sem=back_recv.at[off],
            device_id={"lev": peer},
            device_id_type=MESH,
        )

    def part_copy(off, peer, rank):
        return pltpu.make_async_remote_copy(
            src_ref=part,
            dst_ref=parts.at[rank],
            send_sem=part_send.at[off],
            recv_sem=part_recv.at[off],
            device_id={"lev": peer},
            device_id_type=MESH,
        )

    def cost_copy(off, rank):
        return pltpu.make_async_remote_copy(
            src_ref=costs.at[lon],
            dst_ref=costs.at[rank],
            send_sem=cost_send.at[off],
            recv_sem=cost_recv.at[off],
            device_id={"lon": lons[off]},
            device_id_type=MESH,
        )

    def send_chunk(c, carry):
        for off, peer in enumerate(peers):
            ens_copy(off, peer, me, c).start()
        return carry

    def edges(values):
        lines = values.reshape(values.shape[0] // cols, cols, values.shape[1])
        span = values.shape[0] // cols * half
        to_right = lines[:, cols - half :].reshape(span, values.shape[1]).astype(BF16)
        to_left = lines[:, :half].reshape(span, values.shape[1]).astype(BF16)
        return to_right, to_left

    gather_start(1)
    gather_start(0)
    lax.fori_loop(0, 2 * pairs, send_chunk, 0)
    sbuf[:rows] = spart[...]
    ssend[0], ssend[1] = edges(spart[...].astype(F32))
    for side_to in range(2):
        static_halo(side_to).start()

    lg[me] = lpad[...]
    vg[me] = vsend[...]
    acc[...] = jnp.zeros_like(acc)

    def columns(count, inside):
        col = lax.broadcasted_iota(jnp.int32, (count, inside * 2), 1)
        inner = col < inside
        low = col < inside + inside // 2
        tail = jnp.where(low, col - inside, col - inside - inside // 2)
        level = jnp.where(inner, col // cols, tail // half)
        place = jnp.where(
            inner,
            half + col % cols,
            jnp.where(low, tail % half, half + cols + tail % half),
        )
        return level, place

    def banded(place, weights):
        spot = place - lax.broadcasted_iota(jnp.int32, place.shape, 0)
        tap = weights[...].astype(F32)
        band = jnp.zeros(place.shape, F32)
        for d in range(tap.shape[1]):
            band = jnp.where(spot == d, tap[:, d : d + 1], band)
        return band

    level, place = columns(cols, rows)
    band = banded(place, static_taper)
    for q in range(levs):
        sband[q * cols : (q + 1) * cols] = jnp.where(level == q, band, 0.0).astype(BF16)
    for side_to in range(2):
        static_halo(side_to).wait_recv()
    smooth[...] = jnp.dot(sband[...], sbuf[...], preferred_element_type=F32).astype(BF16)
    zs[slot(me)] = smooth[...]

    @pl.when(gate)
    def _():
        gather_start(2)
        gather_start(3)

    lanes = lpad.shape[1]
    level, place = columns(lanes, full)
    row = lax.broadcasted_iota(jnp.int32, (lanes, wide), 0)
    pick[...] = jnp.where(row == level, 1.0, 0.0).astype(BF16)
    tband[...] = banded(place[:cols], taper)

    padrows = lpad.shape[0]

    gather_far(1)
    gather_far(0)
    gather_near(1)
    gather_near(0)
    fbuf[...] = fgroup[...].astype(F32)

    def expand_loc(rank, carry):
        spread[...] = jnp.dot(lg[rank], pick[...], preferred_element_type=F32)

        def one(q, inner_carry):
            at = pl.ds(pl.multiple_of((rank * levs + q) * cols, 16), cols)
            w[at] = (spread[pl.ds(q, 1)] * tband[...]).astype(BF16)
            return inner_carry

        return lax.fori_loop(0, levs, one, carry)

    lax.fori_loop(0, nlev, expand_loc, 0)
    spread[:, :full] = jnp.dot(spad[...], pick[:, :full], preferred_element_type=F32)
    same = lax.broadcasted_iota(jnp.int32, (cols, full), 1) % cols == (
        lax.broadcasted_iota(jnp.int32, (cols, full), 0)
    )

    def expand_static(q, carry):
        at = pl.ds(pl.multiple_of(q * cols, 16), cols)
        ws[at] = jnp.where(same, spread[pl.ds(q, 1), :full], 0.0).astype(BF16)
        return carry

    lax.fori_loop(0, levs, expand_static, 0)

    nby = lats // GROUP
    nbx = cols // LINE
    levels = nlev * levs
    live = ids[...] >= 0
    local_ids = ids[...] - lon * (nbx * nby)
    by = jnp.where(live, local_ids % nby, -1)
    bx = jnp.where(live, local_ids // nby, -1)
    hturn[...] = horiz[...].T

    def spread_horiz(s, carry):
        line = hturn[pl.ds(pl.multiple_of(s * GROUP, GROUP), GROUP)]
        block = jnp.concatenate([jnp.where(by == q, line, 0.0) for q in range(nby)], axis=0)
        at = pl.ds(pl.multiple_of(s * lats, lats), lats)
        hcol[at] = block.astype(BF16)
        hrow[:, at] = block.T.astype(BF16)
        return carry

    lax.fori_loop(0, LINE, spread_horiz, 0)

    own_copy.wait()

    tile = full // 3 if full % 48 == 0 else full

    def enter(c, h, rank):
        lane = slice(h * 128, (h + 1) * 128)
        product = ebuf[2 * c + h, slot(rank)].astype(F32) * fbuf[slot(rank)]
        at = pl.ds(pl.multiple_of(rank * strip, 16), strip)
        hsend[0, c, at, lane], hsend[1, c, at, lane] = edges(product)
        zbuf[c, slot(rank), lane] = product.astype(BF16)
        for side_to in range(2):
            halo_copy(side_to, c, h, rank).start()

    gates = (hl - 1, hl)

    def arrive(c, h, rank):
        ens_copy(0, peers[0], rank, 2 * c + h).wait_recv()

    def chunk(t, carry):
        @pl.when(t < pairs)
        def _():
            for h in range(2):
                enter(t, h, me)
                for rank in range(nlev):
                    if rank not in gates:

                        @pl.when(rank != me)
                        def _(h=h, rank=rank):
                            arrive(t, h, rank)
                            enter(t, h, rank)

        c = t - lead

        @pl.when((c >= 0) & (c < pairs))
        def _():
            for h in range(2):
                for rank in gates:

                    @pl.when(rank != me)
                    def _(h=h, rank=rank):
                        arrive(c, h, rank)
                        enter(c, h, rank)

                if h == 0:

                    @pl.when((c == pairs - 1) & jnp.logical_not(gate))
                    def _():
                        gather_start(2)
                        gather_start(3)

        @pl.when((c == pairs) & gate)
        def _():
            gather_far(2)
            gather_far(3)

        @pl.when(c >= 1)
        def _():
            d = c - 1
            for h in range(2):
                for side_to in range(2):
                    halo_copy(side_to, d, h).wait_recv()

            def piece(q, inner_carry):
                at = pl.ds(pl.multiple_of(q * tile, 16), tile)
                zv = jnp.dot(w[at], zbuf[d], preferred_element_type=F32)
                acc[at] += (
                    ebuf[2 * d, at].astype(F32) * zv[:, :128]
                    + ebuf[2 * d + 1, at].astype(F32) * zv[:, 128:]
                )
                return inner_carry

            lax.fori_loop(0, full // tile, piece, 0)

        return carry

    lax.fori_loop(0, pairs + lead + 1, chunk, 0)

    accb[...] = acc[...].astype(BF16)
    for off, peer in enumerate(peers):
        back_copy(off, peer).start()

    @pl.when(jnp.logical_not(gate))
    def _():
        gather_far(2)
        gather_far(3)

    gather_near(2)
    gather_near(3)
    for rank in range(nlev):
        folded = vg[rank].astype(F32)
        for p in range(folds):
            piece = folded[p * levs : (p + 1) * levs]
            lane = slice(p * 128, (p + 1) * 128)
            for q in range(nbx):
                at = slice(q * levels + rank * levs, q * levels + (rank + 1) * levs)
                vx[at, lane] = jnp.where(bx[:, lane] == q, piece, 0.0)
    static = jnp.dot(ws[...], zs[...], preferred_element_type=F32)
    acc[slot(me)] += (static_weight / ens_weight) * sdev[...] * static

    for q in range(nbx):
        for s in range(LINE):
            cells[q * levels : (q + 1) * levels, s * lats : (s + 1) * lats] = acc[
                pl.ds(q * LINE + s, levels, stride=cols)
            ]
    projected = jnp.dot(cells[...].astype(BF16), hcol[...], preferred_element_type=F32)
    mine = ens_weight * jnp.sum(projected * vx[...], axis=0, keepdims=True)
    part[...] = mine
    parts[me] = mine
    for off, peer in enumerate(peers):
        part_copy(off, peer, me).start()
    for off, rank in enumerate(sources):
        part_copy(off, peers[off], rank).wait_recv()
    hx = parts[0]
    for rank in range(1, nlev):
        hx = hx + parts[rank]
    miss = hx - value[...]
    dep = jnp.where(live, rinv[...] * miss, 0.0)
    terms = 0.5 * dep * miss
    folded = terms[:, :128]
    for q in range(1, slots // 128):
        folded = folded + terms[:, q * 128 : (q + 1) * 128]
    costs[lon] = folded
    for off in range(nlon - 1):
        cost_copy(off, lon).start()
    held = -(-levs // 8) * 8
    weighted = jnp.concatenate(
        [vert[...] * (dep / ens_weight), jnp.zeros((held - levs, slots), F32)], axis=0
    )
    chosen = jnp.concatenate([jnp.where(bx == q, weighted, 0.0) for q in range(nbx)], axis=0)
    sums = jnp.dot(chosen.astype(BF16), hrow[...], preferred_element_type=F32)
    for q in range(nbx):
        for s in range(LINE):
            both[1, pl.ds(q * LINE + s, levs, stride=cols)] = sums[
                q * held : q * held + levs, s * lats : (s + 1) * lats
            ]
    total = acc[slot(me)]
    for off, peer in enumerate(peers):
        back_copy(off, peer).wait_recv()
        total = total + rbuf[off].astype(F32)
    both[0] = total
    for off in range(nlon - 1):
        cost_copy(off, lax.rem(lon + nlon - off - 1, nlon)).wait_recv()
    total_cost = costs[0]
    for rank in range(1, nlon):
        total_cost = total_cost + costs[rank]
    cost[...] = jnp.sum(total_cost, axis=1, keepdims=True)

    for off, peer in enumerate(peers):
        part_copy(off, peer, me).wait_send()
    for off in range(nlon - 1):
        cost_copy(off, lon).wait_send()
    for which in range(4):
        gather_drain(which)
    for off, peer in enumerate(peers):
        back_copy(off, peer).wait_send()
    for side_to in range(2):
        static_halo(side_to).wait_send()

    def drain(c, carry):
        for h in range(2):
            for off, peer in enumerate(peers):
                ens_copy(off, peer, me, 2 * c + h).wait_send()
            for side_to in range(2):
                halo_copy(side_to, c, h).wait_send()
        return carry

    lax.fori_loop(0, pairs, drain, 0)


def body(
    nlev,
    nlon,
    field,
    ens,
    sdev,
    lon_taper,
    static_taper,
    loc_vert,
    static_vert,
    obs_block,
    obs_value,
    obs_rinv,
    obs_horiz,
    obs_vert,
):
    members, levs, cols, lats = ens.shape
    half = lon_taper.shape[0] // 2
    pairs = members // nlev // 2
    rows = levs * cols
    full = nlev * rows
    edge = nlev * levs * half
    wide = full + 2 * edge
    slots = obs_block.shape[0]
    padrows = -(-levs // 16) * 16
    taps = lon_taper.shape[0]
    width = loc_vert.shape[1]
    picks = cols // LINE * nlev * levs
    hl = nlev // 2
    vmem = pl.BlockSpec(memory_space=pltpu.VMEM)
    dma = pltpu.SemaphoreType.DMA
    both, obs_cost = pl.pallas_call(
        functools.partial(main_kernel, (nlev, nlon, levs, cols, half, pairs)),
        out_shape=(
            jax.ShapeDtypeStruct((2, rows, lats), F32),
            jax.ShapeDtypeStruct((1, 1), F32),
        ),
        in_specs=[pl.BlockSpec(memory_space=pl.ANY)] * 12,
        out_specs=(vmem, vmem),
        scratch_shapes=[
            pltpu.VMEM((rows, lats), F32),
            pltpu.VMEM((rows, lats), F32),
            pltpu.VMEM((1, taps), BF16),
            pltpu.VMEM((1, taps), BF16),
            pltpu.VMEM((levs, width), BF16),
            pltpu.VMEM((levs, width), BF16),
            pltpu.VMEM((1, slots), jnp.int32),
            pltpu.VMEM((1, slots), F32),
            pltpu.VMEM((1, slots), F32),
            pltpu.VMEM((slots, lats), F32),
            pltpu.VMEM((levs, slots), F32),
            pltpu.VMEM((2 * pairs, full, lats), BF16),
            pltpu.VMEM((pairs, wide, 2 * lats), BF16),
            pltpu.VMEM((2, pairs, edge, 2 * lats), BF16),
            pltpu.VMEM((rows, lats), BF16),
            pltpu.VMEM((full, lats), BF16),
            pltpu.VMEM((full, lats), F32),
            pltpu.VMEM((rows, lats), BF16),
            pltpu.VMEM((rows, 2 * rows), BF16),
            pltpu.VMEM((2 * rows, lats), BF16),
            pltpu.VMEM((2, levs * half, lats), BF16),
            pltpu.VMEM((rows, lats), BF16),
            pltpu.VMEM((full, lats), BF16),
            pltpu.VMEM((padrows, 128), BF16),
            pltpu.VMEM((padrows, 128), BF16),
            pltpu.VMEM((nlev, padrows, 128), BF16),
            pltpu.VMEM((padrows, wide), F32),
            pltpu.VMEM((full, wide), BF16),
            pltpu.VMEM((rows, full), BF16),
            pltpu.VMEM((128, wide), BF16),
            pltpu.VMEM((cols, wide), F32),
            pltpu.VMEM((full, lats), F32),
            pltpu.VMEM((full, lats), BF16),
            pltpu.VMEM((nlev - 1, rows, lats), BF16),
            pltpu.VMEM((lats, slots), F32),
            pltpu.VMEM((LINE * lats, slots), BF16),
            pltpu.VMEM((slots, LINE * lats), BF16),
            pltpu.VMEM((picks, LINE * lats), F32),
            pltpu.VMEM((levs * slots // 128, 128), F32),
            pltpu.VMEM((levs * slots // 128, 128), BF16),
            pltpu.VMEM((nlev, levs * slots // 128, 128), BF16),
            pltpu.VMEM((picks, slots), F32),
            pltpu.VMEM((1, slots), F32),
            pltpu.VMEM((nlev, 1, slots), F32),
            pltpu.VMEM((nlon, 1, 128), F32),
            dma,
            dma((11,)),
            dma((nlev - 1, 2 * pairs)),
            dma((nlev, 2 * pairs)),
            dma((2, 2 * pairs + 1)),
            dma((2, 2 * pairs + 1)),
            dma((4, nlev - 1)),
            dma((4, nlev)),
            dma((4, hl * hl)),
            dma((nlev - 1,)),
            dma((nlev - 1,)),
            dma((nlev - 1,)),
            dma((nlev - 1,)),
            dma((nlon - 1,)),
            dma((nlon - 1,)),
        ],
        compiler_params=pltpu.CompilerParams(
            collective_id=0, has_side_effects=True, vmem_limit_bytes=63 * 1024 * 1024
        ),
        name="covariance",
    )(
        ens.reshape(members, rows, lats),
        field.reshape(rows, lats),
        sdev.reshape(rows, lats),
        lon_taper.reshape(1, -1),
        static_taper.reshape(1, -1),
        loc_vert,
        static_vert,
        obs_block.reshape(1, slots),
        obs_value.reshape(1, slots),
        obs_rinv.reshape(1, slots),
        obs_horiz,
        obs_vert.T,
    )
    shape = (levs, cols, lats)
    increment, adjoint_field = ens_weight * both[0], ens_weight * both[1]
    return (increment.reshape(shape), adjoint_field.reshape(shape), obs_cost[0, 0])


def solution(mesh):
    return jax.shard_map(
        functools.partial(body, mesh.shape["lev"], mesh.shape["lon"]),
        mesh=mesh,
        in_specs=(
            P("lev", "lon", None),
            P(None, "lev", "lon", None),
            P("lev", "lon", None),
            P(),
            P(),
            P("lev", None),
            P("lev", None),
            P("lon"),
            P("lon"),
            P("lon"),
            P("lon", None),
            P("lon", "lev"),
        ),
        out_specs=(P("lev", "lon", None), P("lev", "lon", None), P()),
        check_vma=False,
    )
```

```python
import functools

import jax
import jax.numpy as jnp
from jax import lax
from jax.experimental import pallas as pl
from jax.experimental.pallas import tpu as pltpu
from jax.sharding import PartitionSpec as P

ens_weight = 0.8
static_weight = 0.5
MESH = pl.DeviceIdType.MESH
F32 = jnp.float32
BF16 = jnp.bfloat16


LINE = 8
GROUP = 16


def main_kernel(
    dims,
    ens,
    field_in,
    sdev_in,
    taper_in,
    static_taper_in,
    loc_in,
    svert_in,
    ids_in,
    value_in,
    rinv_in,
    horiz_in,
    vert_in,
    both,
    cost,
    field,
    sdev,
    taper,
    static_taper,
    loc,
    svert,
    ids,
    value,
    rinv,
    horiz,
    vert,
    ebuf,
    zbuf,
    hsend,
    fsend,
    fgroup,
    fbuf,
    spart,
    sband,
    sbuf,
    ssend,
    smooth,
    zs,
    lpad,
    spad,
    lg,
    spread,
    w,
    ws,
    pick,
    tband,
    acc,
    accb,
    rbuf,
    hturn,
    hcol,
    hrow,
    cells,
    vfold,
    vsend,
    vg,
    vx,
    part,
    parts,
    costs,
    own_sem,
    in_sem,
    ens_send,
    ens_recv,
    halo_send,
    halo_recv,
    small_send,
    small_recv,
    relay_send,
    back_send,
    back_recv,
    part_send,
    part_recv,
    cost_send,
    cost_recv,
):
    nlev, nlon, levs, cols, half, pairs = dims
    rows = levs * cols
    full = nlev * rows
    edge = nlev * levs * half
    wide = full + 2 * edge
    strip = levs * half
    hl = nlev // 2
    me = lax.axis_index("lev")
    lon = lax.axis_index("lon")
    right, left = lax.rem(lon + 1, nlon), lax.rem(lon + nlon - 1, nlon)
    peers = [lax.rem(me + off, nlev) for off in range(1, nlev)]
    sources = [lax.rem(me + nlev - off, nlev) for off in range(1, nlev)]
    side = me // hl
    gate = (me == hl - 1) | (me == hl)
    other_gate = hl - 1 + (1 - side)
    far_ranks = [(1 - side) * hl + q for q in range(hl)]
    near_ranks = [side * hl + lax.rem(me - side * hl + q, hl) for q in range(1, hl)]

    def slot(rank):
        return pl.ds(pl.multiple_of(rank * rows, 16), rows)

    own_copy = pltpu.make_async_copy(
        ens.at[pl.ds(me * 2 * pairs, 2 * pairs)], ebuf.at[:, slot(me)], own_sem
    )
    staged = (
        (field_in, field),
        (loc_in, loc),
        (svert_in, svert),
        (taper_in, taper),
        (static_taper_in, static_taper),
        (sdev_in, sdev),
        (ids_in, ids),
        (value_in, value),
        (rinv_in, rinv),
        (horiz_in, horiz),
        (vert_in, vert),
    )
    stage = [
        pltpu.make_async_copy(src, dst, in_sem.at[q]) for q, (src, dst) in enumerate(staged)
    ]
    for copy in stage:
        copy.start()
    own_copy.start()
    lons = [lax.rem(lon + off, nlon) for off in range(1, nlon)]

    barrier = pltpu.get_barrier_semaphore()
    for peer in peers:
        pl.semaphore_signal(barrier, inc=1, device_id={"lev": peer}, device_id_type=MESH)
    for peer in lons:
        pl.semaphore_signal(barrier, inc=1, device_id={"lon": peer}, device_id_type=MESH)
    width = loc.shape[1]
    stage[0].wait()
    fsend[...] = field[...].astype(BF16)
    fgroup[slot(me)] = fsend[...]
    for copy in stage[1:]:
        copy.wait()
    for matrix, padded in ((loc, lpad), (svert, spad)):
        padded[...] = jnp.zeros_like(padded)
        padded[:levs, :width] = matrix[...]
    spart[...] = (sdev[...] * field[...]).astype(BF16)
    slots = ids.shape[1]
    lats = field.shape[1]
    folds = slots // 128
    for q in range(folds):
        vfold[q * levs : (q + 1) * levs] = vert[:, q * 128 : (q + 1) * 128]
    vsend[...] = vfold[...].astype(BF16)
    pl.semaphore_wait(barrier, nlev + nlon - 2)

    def land(which, rank):
        dst = (lg, fgroup, zs, vg)[which]
        return dst.at[rank] if which in (0, 3) else dst.at[slot(rank)]

    def small(which, off, peer, rank):
        return pltpu.make_async_remote_copy(
            src_ref=(lpad, fsend, smooth, vsend)[which],
            dst_ref=land(which, rank),
            send_sem=small_send.at[which, off],
            recv_sem=small_recv.at[which, rank],
            device_id={"lev": peer},
            device_id_type=MESH,
        )

    def relay(which, q, k):
        return pltpu.make_async_remote_copy(
            src_ref=land(which, far_ranks[q]),
            dst_ref=land(which, far_ranks[q]),
            send_sem=relay_send.at[which, q * hl + k],
            recv_sem=small_recv.at[which, far_ranks[q]],
            device_id={"lev": near_ranks[k]},
            device_id_type=MESH,
        )

    def gather_start(which):
        for off, peer in enumerate(peers):

            @pl.when((peer // hl == side) | (peer == other_gate))
            def _(off=off, peer=peer):
                small(which, off, peer, me).start()

    def gather_far(which):
        for q, rank in enumerate(far_ranks):
            small(which, 0, peers[0], rank).wait_recv()

            @pl.when(gate)
            def _(q=q):
                for k in range(hl - 1):
                    relay(which, q, k).start()

    def gather_near(which):
        for rank in near_ranks:
            small(which, 0, peers[0], rank).wait_recv()

    def gather_drain(which):
        for off, peer in enumerate(peers):

            @pl.when((peer // hl == side) | (peer == other_gate))
            def _(off=off, peer=peer):
                small(which, off, peer, me).wait_send()

        @pl.when(gate)
        def _():
            for q in range(hl):
                for k in range(hl - 1):
                    relay(which, q, k).wait_send()

    def ens_copy(off, peer, rank, c):
        return pltpu.make_async_remote_copy(
            src_ref=ens.at[peer * 2 * pairs + c],
            dst_ref=ebuf.at[c, slot(rank)],
            send_sem=ens_send.at[off, c],
            recv_sem=ens_recv.at[rank, c],
            device_id={"lev": peer},
            device_id_type=MESH,
        )

    def halo_copy(side_to, c, h, rank=None):
        lane = pl.ds(pl.multiple_of(h * 128, 128), 128)
        base = full + side_to * edge
        if rank is None:
            src, dst = pl.ds(0, edge), pl.ds(base, edge)
        else:
            first = pl.multiple_of(rank * strip, 16)
            src, dst = pl.ds(first, strip), pl.ds(base + first, strip)
        return pltpu.make_async_remote_copy(
            src_ref=hsend.at[side_to, c, src, lane],
            dst_ref=zbuf.at[c, dst, lane],
            send_sem=halo_send.at[side_to, 2 * c + h],
            recv_sem=halo_recv.at[side_to, 2 * c + h],
            device_id={"lon": (right, left)[side_to]},
            device_id_type=MESH,
        )

    def static_halo(side_to):
        return pltpu.make_async_remote_copy(
            src_ref=ssend.at[side_to],
            dst_ref=sbuf.at[pl.ds(rows + side_to * strip, strip)],
            send_sem=halo_send.at[side_to, 2 * pairs],
            recv_sem=halo_recv.at[side_to, 2 * pairs],
            device_id={"lon": (right, left)[side_to]},
            device_id_type=MESH,
        )

    def back_copy(off, peer):
        return pltpu.make_async_remote_copy(
            src_ref=accb.at[slot(peer)],
            dst_ref=rbuf.at[off],
            send_sem=back_send.at[off],
            recv_sem=back_recv.at[off],
            device_id={"lev": peer},
            device_id_type=MESH,
        )

    def part_copy(off, peer, rank):
        return pltpu.make_async_remote_copy(
            src_ref=part,
            dst_ref=parts.at[rank],
            send_sem=part_send.at[off],
            recv_sem=part_recv.at[off],
            device_id={"lev": peer},
            device_id_type=MESH,
        )

    def cost_copy(off, rank):
        return pltpu.make_async_remote_copy(
            src_ref=costs.at[lon],
            dst_ref=costs.at[rank],
            send_sem=cost_send.at[off],
            recv_sem=cost_recv.at[off],
            device_id={"lon": lons[off]},
            device_id_type=MESH,
        )

    def send_chunk(c, carry):
        for off, peer in enumerate(peers):
            ens_copy(off, peer, me, c).start()
        return carry

    def edges(values):
        lines = values.reshape(values.shape[0] // cols, cols, values.shape[1])
        span = values.shape[0] // cols * half
        to_right = lines[:, cols - half :].reshape(span, values.shape[1]).astype(BF16)
        to_left = lines[:, :half].reshape(span, values.shape[1]).astype(BF16)
        return to_right, to_left

    gather_start(1)
    gather_start(0)
    gather_start(3)
    lax.fori_loop(0, 2 * pairs, send_chunk, 0)
    sbuf[:rows] = spart[...]
    ssend[0], ssend[1] = edges(spart[...].astype(F32))
    for side_to in range(2):
        static_halo(side_to).start()

    lg[me] = lpad[...]
    vg[me] = vsend[...]
    acc[...] = jnp.zeros_like(acc)

    def columns(count, inside):
        col = lax.broadcasted_iota(jnp.int32, (count, inside * 2), 1)
        inner = col < inside
        low = col < inside + inside // 2
        tail = jnp.where(low, col - inside, col - inside - inside // 2)
        level = jnp.where(inner, col // cols, tail // half)
        place = jnp.where(
            inner,
            half + col % cols,
            jnp.where(low, tail % half, half + cols + tail % half),
        )
        return level, place

    def banded(place, weights):
        spot = place - lax.broadcasted_iota(jnp.int32, place.shape, 0)
        tap = weights[...].astype(F32)
        band = jnp.zeros(place.shape, F32)
        for d in range(tap.shape[1]):
            band = jnp.where(spot == d, tap[:, d : d + 1], band)
        return band

    level, place = columns(cols, rows)
    band = banded(place, static_taper)
    for q in range(levs):
        sband[q * cols : (q + 1) * cols] = jnp.where(level == q, band, 0.0).astype(BF16)
    for side_to in range(2):
        static_halo(side_to).wait_recv()
    smooth[...] = jnp.dot(sband[...], sbuf[...], preferred_element_type=F32).astype(BF16)
    zs[slot(me)] = smooth[...]

    @pl.when(gate)
    def _():
        gather_start(2)

    lanes = lpad.shape[1]
    level, place = columns(lanes, full)
    row = lax.broadcasted_iota(jnp.int32, (lanes, wide), 0)
    pick[...] = jnp.where(row == level, 1.0, 0.0).astype(BF16)
    tband[...] = banded(place[:cols], taper)

    padrows = lpad.shape[0]

    gather_far(1)
    gather_far(0)
    gather_near(1)
    gather_near(0)
    fbuf[...] = fgroup[...].astype(F32)

    def expand_loc(rank, carry):
        spread[...] = jnp.dot(lg[rank], pick[...], preferred_element_type=F32)

        def one(q, inner_carry):
            at = pl.ds(pl.multiple_of((rank * levs + q) * cols, 16), cols)
            w[at] = (spread[pl.ds(q, 1)] * tband[...]).astype(BF16)
            return inner_carry

        return lax.fori_loop(0, levs, one, carry)

    lax.fori_loop(0, nlev, expand_loc, 0)
    spread[:, :full] = jnp.dot(spad[...], pick[:, :full], preferred_element_type=F32)
    same = lax.broadcasted_iota(jnp.int32, (cols, full), 1) % cols == (
        lax.broadcasted_iota(jnp.int32, (cols, full), 0)
    )

    def expand_static(q, carry):
        at = pl.ds(pl.multiple_of(q * cols, 16), cols)
        ws[at] = jnp.where(same, spread[pl.ds(q, 1), :full], 0.0).astype(BF16)
        return carry

    lax.fori_loop(0, levs, expand_static, 0)

    nby = lats // GROUP
    nbx = cols // LINE
    levels = nlev * levs
    live = ids[...] >= 0
    local_ids = ids[...] - lon * (nbx * nby)
    by = jnp.where(live, local_ids % nby, -1)
    bx = jnp.where(live, local_ids // nby, -1)
    hturn[...] = horiz[...].T

    def spread_horiz(s, carry):
        line = hturn[pl.ds(pl.multiple_of(s * GROUP, GROUP), GROUP)]
        block = jnp.concatenate([jnp.where(by == q, line, 0.0) for q in range(nby)], axis=0)
        at = pl.ds(pl.multiple_of(s * lats, lats), lats)
        hcol[at] = block.astype(BF16)
        hrow[:, at] = block.T.astype(BF16)
        return carry

    lax.fori_loop(0, LINE, spread_horiz, 0)

    gather_far(3)
    gather_near(3)
    for rank in range(nlev):
        folded = vg[rank].astype(F32)
        for p in range(folds):
            piece = folded[p * levs : (p + 1) * levs]
            lane = slice(p * 128, (p + 1) * 128)
            for q in range(nbx):
                at = slice(q * levels + rank * levs, q * levels + (rank + 1) * levs)
                vx[at, lane] = jnp.where(bx[:, lane] == q, piece, 0.0)

    own_copy.wait()

    tile = full // 3 if full % 48 == 0 else full

    steps = 2 * nlev

    def enter(e, c):
        late = e >= steps
        h = jnp.where(late, (e - steps) // 2, e // nlev)
        rank = jnp.where(late, hl - 1 + (e - steps) % 2, e % nlev)
        gated = (rank == hl - 1) | (rank == hl)
        mine = rank == me

        @pl.when(jnp.where(late, jnp.logical_not(mine), jnp.logical_not(gated) | mine))
        def _():
            @pl.when(jnp.logical_not(mine))
            def _():
                ens_copy(0, peers[0], rank, 2 * c + h).wait_recv()

            lane = pl.ds(pl.multiple_of(h * 128, 128), 128)
            product = ebuf[2 * c + h, slot(rank)].astype(F32) * fbuf[slot(rank)]
            at = pl.ds(pl.multiple_of(rank * strip, 16), strip)
            hsend[0, c, at, lane], hsend[1, c, at, lane] = edges(product)
            zbuf[c, slot(rank), lane] = product.astype(BF16)
            for side_to in range(2):
                halo_copy(side_to, c, h, rank).start()

        return c

    def chunk(c, carry):
        @pl.when(c < pairs)
        def _():
            lax.fori_loop(0, steps + 4, enter, c)

            @pl.when((c == pairs - 1) & jnp.logical_not(gate))
            def _():
                gather_start(2)

        @pl.when((c == pairs) & gate)
        def _():
            gather_far(2)

        @pl.when(c >= 1)
        def _():
            d = c - 1
            for h in range(2):
                for side_to in range(2):
                    halo_copy(side_to, d, h).wait_recv()

            def piece(q, inner_carry):
                at = pl.ds(pl.multiple_of(q * tile, 16), tile)
                zv = jnp.dot(w[at], zbuf[d], preferred_element_type=F32)
                acc[at] += (
                    ebuf[2 * d, at].astype(F32) * zv[:, :128]
                    + ebuf[2 * d + 1, at].astype(F32) * zv[:, 128:]
                )
                return inner_carry

            lax.fori_loop(0, full // tile, piece, 0)

        return carry

    lax.fori_loop(0, pairs + 1, chunk, 0)

    @pl.when(jnp.logical_not(gate))
    def _():
        gather_far(2)

    gather_near(2)
    static = jnp.dot(ws[...], zs[...], preferred_element_type=F32)
    acc[slot(me)] += (static_weight / ens_weight) * sdev[...] * static

    for q in range(nbx):
        for s in range(LINE):
            cells[q * levels : (q + 1) * levels, s * lats : (s + 1) * lats] = acc[
                pl.ds(q * LINE + s, levels, stride=cols)
            ]
    projected = jnp.dot(cells[...].astype(BF16), hcol[...], preferred_element_type=F32)
    mine = ens_weight * jnp.sum(projected * vx[...], axis=0, keepdims=True)
    part[...] = mine
    parts[me] = mine
    for off, peer in enumerate(peers):
        part_copy(off, peer, me).start()
    accb[...] = acc[...].astype(BF16)
    for off, peer in enumerate(peers):
        back_copy(off, peer).start()
    for off, rank in enumerate(sources):
        part_copy(off, peers[off], rank).wait_recv()
    hx = parts[0]
    for rank in range(1, nlev):
        hx = hx + parts[rank]
    miss = hx - value[...]
    dep = jnp.where(live, rinv[...] * miss, 0.0)
    terms = 0.5 * dep * miss
    folded = terms[:, :128]
    for q in range(1, slots // 128):
        folded = folded + terms[:, q * 128 : (q + 1) * 128]
    costs[lon] = folded
    for off in range(nlon - 1):
        cost_copy(off, lon).start()
    held = -(-levs // 8) * 8
    weighted = jnp.concatenate(
        [vert[...] * (dep / ens_weight), jnp.zeros((held - levs, slots), F32)], axis=0
    )
    chosen = jnp.concatenate([jnp.where(bx == q, weighted, 0.0) for q in range(nbx)], axis=0)
    sums = jnp.dot(chosen.astype(BF16), hrow[...], preferred_element_type=F32)
    for q in range(nbx):
        for s in range(LINE):
            both[1, pl.ds(q * LINE + s, levs, stride=cols)] = sums[
                q * held : q * held + levs, s * lats : (s + 1) * lats
            ]
    total = acc[slot(me)]
    for off, peer in enumerate(peers):
        back_copy(off, peer).wait_recv()
        total = total + rbuf[off].astype(F32)
    both[0] = total
    for off in range(nlon - 1):
        cost_copy(off, lax.rem(lon + nlon - off - 1, nlon)).wait_recv()
    total_cost = costs[0]
    for rank in range(1, nlon):
        total_cost = total_cost + costs[rank]
    cost[...] = jnp.sum(total_cost, axis=1, keepdims=True)

    for off, peer in enumerate(peers):
        part_copy(off, peer, me).wait_send()
    for off in range(nlon - 1):
        cost_copy(off, lon).wait_send()
    for which in range(4):
        gather_drain(which)
    for off, peer in enumerate(peers):
        back_copy(off, peer).wait_send()
    for side_to in range(2):
        static_halo(side_to).wait_send()

    def drain(c, carry):
        for h in range(2):
            for off, peer in enumerate(peers):
                ens_copy(off, peer, me, 2 * c + h).wait_send()
            for side_to in range(2):
                halo_copy(side_to, c, h).wait_send()
        return carry

    lax.fori_loop(0, pairs, drain, 0)


def body(
    nlev,
    nlon,
    field,
    ens,
    sdev,
    lon_taper,
    static_taper,
    loc_vert,
    static_vert,
    obs_block,
    obs_value,
    obs_rinv,
    obs_horiz,
    obs_vert,
):
    members, levs, cols, lats = ens.shape
    half = lon_taper.shape[0] // 2
    pairs = members // nlev // 2
    rows = levs * cols
    full = nlev * rows
    edge = nlev * levs * half
    wide = full + 2 * edge
    slots = obs_block.shape[0]
    padrows = -(-levs // 16) * 16
    taps = lon_taper.shape[0]
    width = loc_vert.shape[1]
    picks = cols // LINE * nlev * levs
    hl = nlev // 2
    vmem = pl.BlockSpec(memory_space=pltpu.VMEM)
    dma = pltpu.SemaphoreType.DMA
    both, obs_cost = pl.pallas_call(
        functools.partial(main_kernel, (nlev, nlon, levs, cols, half, pairs)),
        out_shape=(
            jax.ShapeDtypeStruct((2, rows, lats), F32),
            jax.ShapeDtypeStruct((1, 1), F32),
        ),
        in_specs=[pl.BlockSpec(memory_space=pl.ANY)] * 12,
        out_specs=(vmem, vmem),
        scratch_shapes=[
            pltpu.VMEM((rows, lats), F32),
            pltpu.VMEM((rows, lats), F32),
            pltpu.VMEM((1, taps), BF16),
            pltpu.VMEM((1, taps), BF16),
            pltpu.VMEM((levs, width), BF16),
            pltpu.VMEM((levs, width), BF16),
            pltpu.VMEM((1, slots), jnp.int32),
            pltpu.VMEM((1, slots), F32),
            pltpu.VMEM((1, slots), F32),
            pltpu.VMEM((slots, lats), F32),
            pltpu.VMEM((levs, slots), F32),
            pltpu.VMEM((2 * pairs, full, lats), BF16),
            pltpu.VMEM((pairs, wide, 2 * lats), BF16),
            pltpu.VMEM((2, pairs, edge, 2 * lats), BF16),
            pltpu.VMEM((rows, lats), BF16),
            pltpu.VMEM((full, lats), BF16),
            pltpu.VMEM((full, lats), F32),
            pltpu.VMEM((rows, lats), BF16),
            pltpu.VMEM((rows, 2 * rows), BF16),
            pltpu.VMEM((2 * rows, lats), BF16),
            pltpu.VMEM((2, levs * half, lats), BF16),
            pltpu.VMEM((rows, lats), BF16),
            pltpu.VMEM((full, lats), BF16),
            pltpu.VMEM((padrows, 128), BF16),
            pltpu.VMEM((padrows, 128), BF16),
            pltpu.VMEM((nlev, padrows, 128), BF16),
            pltpu.VMEM((padrows, wide), F32),
            pltpu.VMEM((full, wide), BF16),
            pltpu.VMEM((rows, full), BF16),
            pltpu.VMEM((128, wide), BF16),
            pltpu.VMEM((cols, wide), F32),
            pltpu.VMEM((full, lats), F32),
            pltpu.VMEM((full, lats), BF16),
            pltpu.VMEM((nlev - 1, rows, lats), BF16),
            pltpu.VMEM((lats, slots), F32),
            pltpu.VMEM((LINE * lats, slots), BF16),
            pltpu.VMEM((slots, LINE * lats), BF16),
            pltpu.VMEM((picks, LINE * lats), F32),
            pltpu.VMEM((levs * slots // 128, 128), F32),
            pltpu.VMEM((levs * slots // 128, 128), BF16),
            pltpu.VMEM((nlev, levs * slots // 128, 128), BF16),
            pltpu.VMEM((picks, slots), F32),
            pltpu.VMEM((1, slots), F32),
            pltpu.VMEM((nlev, 1, slots), F32),
            pltpu.VMEM((nlon, 1, 128), F32),
            dma,
            dma((11,)),
            dma((nlev - 1, 2 * pairs)),
            dma((nlev, 2 * pairs)),
            dma((2, 2 * pairs + 1)),
            dma((2, 2 * pairs + 1)),
            dma((4, nlev - 1)),
            dma((4, nlev)),
            dma((4, hl * hl)),
            dma((nlev - 1,)),
            dma((nlev - 1,)),
            dma((nlev - 1,)),
            dma((nlev - 1,)),
            dma((nlon - 1,)),
            dma((nlon - 1,)),
        ],
        compiler_params=pltpu.CompilerParams(
            collective_id=0, has_side_effects=True, vmem_limit_bytes=63 * 1024 * 1024
        ),
        name="covariance",
    )(
        ens.reshape(members, rows, lats),
        field.reshape(rows, lats),
        sdev.reshape(rows, lats),
        lon_taper.reshape(1, -1),
        static_taper.reshape(1, -1),
        loc_vert,
        static_vert,
        obs_block.reshape(1, slots),
        obs_value.reshape(1, slots),
        obs_rinv.reshape(1, slots),
        obs_horiz,
        obs_vert.T,
    )
    shape = (levs, cols, lats)
    increment, adjoint_field = ens_weight * both[0], ens_weight * both[1]
    return (increment.reshape(shape), adjoint_field.reshape(shape), obs_cost[0, 0])


def solution(mesh):
    return jax.shard_map(
        functools.partial(body, mesh.shape["lev"], mesh.shape["lon"]),
        mesh=mesh,
        in_specs=(
            P("lev", "lon", None),
            P(None, "lev", "lon", None),
            P("lev", "lon", None),
            P(),
            P(),
            P("lev", None),
            P("lev", None),
            P("lon"),
            P("lon"),
            P("lon"),
            P("lon", None),
            P("lon", "lev"),
        ),
        out_specs=(P("lev", "lon", None), P("lev", "lon", None), P()),
        check_vma=False,
    )
```

```python
import functools

import jax
import jax.numpy as jnp
from jax import lax
from jax.experimental import pallas as pl
from jax.experimental.pallas import tpu as pltpu
from jax.sharding import PartitionSpec as P

ens_weight = 0.8
static_weight = 0.5
MESH = pl.DeviceIdType.MESH
F32 = jnp.float32
BF16 = jnp.bfloat16


LINE = 8
GROUP = 16


def main_kernel(
    dims,
    ens,
    field_in,
    sdev_in,
    taper_in,
    static_taper_in,
    loc_in,
    svert_in,
    ids_in,
    value_in,
    rinv_in,
    horiz_in,
    vert_in,
    both_out,
    cost,
    field,
    sdev,
    taper,
    static_taper,
    loc,
    svert,
    ids,
    value,
    rinv,
    horiz,
    vert,
    ebuf,
    zbuf,
    hsend,
    fsend,
    fgroup,
    fbuf,
    spart,
    sband,
    sbuf,
    ssend,
    smooth,
    zs,
    lpad,
    spad,
    lg,
    spread,
    w,
    ws,
    pick,
    tband,
    acc,
    accb,
    rbuf,
    hturn,
    hcol,
    hrow,
    cells,
    vfold,
    vsend,
    vg,
    vx,
    part,
    parts,
    costs,
    both,
    own_sem,
    out_sem,
    in_sem,
    ens_send,
    ens_recv,
    halo_send,
    halo_recv,
    small_send,
    small_recv,
    relay_send,
    back_send,
    back_recv,
    part_send,
    part_recv,
    cost_send,
    cost_recv,
):
    nlev, nlon, levs, cols, half, pairs = dims
    rows = levs * cols
    full = nlev * rows
    edge = nlev * levs * half
    wide = full + 2 * edge
    strip = levs * half
    hl = nlev // 2
    me = lax.axis_index("lev")
    lon = lax.axis_index("lon")
    right, left = lax.rem(lon + 1, nlon), lax.rem(lon + nlon - 1, nlon)
    peers = [lax.rem(me + off, nlev) for off in range(1, nlev)]
    sources = [lax.rem(me + nlev - off, nlev) for off in range(1, nlev)]
    side = me // hl
    gate = (me == hl - 1) | (me == hl)
    other_gate = hl - 1 + (1 - side)
    far_ranks = [(1 - side) * hl + q for q in range(hl)]
    near_ranks = [side * hl + lax.rem(me - side * hl + q, hl) for q in range(1, hl)]

    def slot(rank):
        return pl.ds(pl.multiple_of(rank * rows, 16), rows)

    own_copy = pltpu.make_async_copy(
        ens.at[pl.ds(me * 2 * pairs, 2 * pairs)], ebuf.at[:, slot(me)], own_sem
    )
    leave = [
        pltpu.make_async_copy(both.at[q], both_out.at[q], out_sem.at[q]) for q in range(2)
    ]
    staged = (
        (field_in, field),
        (loc_in, loc),
        (svert_in, svert),
        (taper_in, taper),
        (static_taper_in, static_taper),
        (sdev_in, sdev),
        (ids_in, ids),
        (value_in, value),
        (rinv_in, rinv),
        (vert_in, vert),
        (horiz_in, horiz),
    )
    stage = [
        pltpu.make_async_copy(src, dst, in_sem.at[q]) for q, (src, dst) in enumerate(staged)
    ]
    lons = [lax.rem(lon + off, nlon) for off in range(1, nlon)]

    barrier = pltpu.get_barrier_semaphore()
    for peer in peers:
        pl.semaphore_signal(barrier, inc=1, device_id={"lev": peer}, device_id_type=MESH)
    for peer in lons:
        pl.semaphore_signal(barrier, inc=1, device_id={"lon": peer}, device_id_type=MESH)
    for copy in stage[:-1]:
        copy.start()
    width = loc.shape[1]
    stage[0].wait()
    fsend[...] = field[...].astype(BF16)
    fgroup[slot(me)] = fsend[...]
    for copy in stage[1:-1]:
        copy.wait()
    for matrix, padded in ((loc, lpad), (svert, spad)):
        padded[...] = jnp.zeros_like(padded)
        padded[:levs, :width] = matrix[...]
    spart[...] = (sdev[...] * field[...]).astype(BF16)
    slots = ids.shape[1]
    lats = field.shape[1]
    folds = slots // 128
    for q in range(folds):
        vfold[q * levs : (q + 1) * levs] = vert[:, q * 128 : (q + 1) * 128]
    vsend[...] = vfold[...].astype(BF16)
    pl.semaphore_wait(barrier, nlev + nlon - 2)

    def land(which, rank):
        dst = (lg, fgroup, zs, vg)[which]
        return dst.at[rank] if which in (0, 3) else dst.at[slot(rank)]

    def small(which, off, peer, rank):
        return pltpu.make_async_remote_copy(
            src_ref=(lpad, fsend, smooth, vsend)[which],
            dst_ref=land(which, rank),
            send_sem=small_send.at[which, off],
            recv_sem=small_recv.at[which, rank],
            device_id={"lev": peer},
            device_id_type=MESH,
        )

    def relay(which, q, k):
        return pltpu.make_async_remote_copy(
            src_ref=land(which, far_ranks[q]),
            dst_ref=land(which, far_ranks[q]),
            send_sem=relay_send.at[which, q * hl + k],
            recv_sem=small_recv.at[which, far_ranks[q]],
            device_id={"lev": near_ranks[k]},
            device_id_type=MESH,
        )

    def gather_start(which):
        for off, peer in enumerate(peers):

            @pl.when((peer // hl == side) | (peer == other_gate))
            def _(off=off, peer=peer):
                small(which, off, peer, me).start()

    def gather_far(which):
        for q, rank in enumerate(far_ranks):
            small(which, 0, peers[0], rank).wait_recv()

            @pl.when(gate)
            def _(q=q):
                for k in range(hl - 1):
                    relay(which, q, k).start()

    def gather_near(which):
        for rank in near_ranks:
            small(which, 0, peers[0], rank).wait_recv()

    def gather_drain(which):
        for off, peer in enumerate(peers):

            @pl.when((peer // hl == side) | (peer == other_gate))
            def _(off=off, peer=peer):
                small(which, off, peer, me).wait_send()

        @pl.when(gate)
        def _():
            for q in range(hl):
                for k in range(hl - 1):
                    relay(which, q, k).wait_send()

    def ens_copy(off, peer, rank, c):
        return pltpu.make_async_remote_copy(
            src_ref=ens.at[peer * 2 * pairs + c],
            dst_ref=ebuf.at[c, slot(rank)],
            send_sem=ens_send.at[off, c],
            recv_sem=ens_recv.at[rank, c],
            device_id={"lev": peer},
            device_id_type=MESH,
        )

    def halo_copy(side_to, c, h, rank=None):
        lane = pl.ds(pl.multiple_of(h * 128, 128), 128)
        base = full + side_to * edge
        if rank is None:
            src, dst = pl.ds(0, edge), pl.ds(base, edge)
        else:
            first = pl.multiple_of(rank * strip, 16)
            src, dst = pl.ds(first, strip), pl.ds(base + first, strip)
        return pltpu.make_async_remote_copy(
            src_ref=hsend.at[side_to, c, src, lane],
            dst_ref=zbuf.at[c, dst, lane],
            send_sem=halo_send.at[side_to, 2 * c + h],
            recv_sem=halo_recv.at[side_to, 2 * c + h],
            device_id={"lon": (right, left)[side_to]},
            device_id_type=MESH,
        )

    def static_halo(side_to):
        return pltpu.make_async_remote_copy(
            src_ref=ssend.at[side_to],
            dst_ref=sbuf.at[pl.ds(rows + side_to * strip, strip)],
            send_sem=halo_send.at[side_to, 2 * pairs],
            recv_sem=halo_recv.at[side_to, 2 * pairs],
            device_id={"lon": (right, left)[side_to]},
            device_id_type=MESH,
        )

    def back_copy(off, peer):
        return pltpu.make_async_remote_copy(
            src_ref=accb.at[slot(peer)],
            dst_ref=rbuf.at[off],
            send_sem=back_send.at[off],
            recv_sem=back_recv.at[off],
            device_id={"lev": peer},
            device_id_type=MESH,
        )

    def part_copy(off, peer, rank):
        return pltpu.make_async_remote_copy(
            src_ref=part,
            dst_ref=parts.at[rank],
            send_sem=part_send.at[off],
            recv_sem=part_recv.at[off],
            device_id={"lev": peer},
            device_id_type=MESH,
        )

    def cost_copy(off, rank):
        return pltpu.make_async_remote_copy(
            src_ref=costs.at[lon],
            dst_ref=costs.at[rank],
            send_sem=cost_send.at[off],
            recv_sem=cost_recv.at[off],
            device_id={"lon": lons[off]},
            device_id_type=MESH,
        )

    def send_chunk(c, carry):
        for off, peer in enumerate(peers):
            ens_copy(off, peer, me, c).start()
        return carry

    def edges(values):
        lines = values.reshape(values.shape[0] // cols, cols, values.shape[1])
        span = values.shape[0] // cols * half
        to_right = lines[:, cols - half :].reshape(span, values.shape[1]).astype(BF16)
        to_left = lines[:, :half].reshape(span, values.shape[1]).astype(BF16)
        return to_right, to_left

    gather_start(1)
    gather_start(0)
    gather_start(3)
    lax.fori_loop(0, 2 * pairs, send_chunk, 0)
    stage[-1].start()
    own_copy.start()
    sbuf[:rows] = spart[...]
    ssend[0], ssend[1] = edges(spart[...].astype(F32))
    for side_to in range(2):
        static_halo(side_to).start()

    lg[me] = lpad[...]
    vg[me] = vsend[...]
    acc[...] = jnp.zeros_like(acc)

    def columns(count, inside):
        col = lax.broadcasted_iota(jnp.int32, (count, inside * 2), 1)
        inner = col < inside
        low = col < inside + inside // 2
        tail = jnp.where(low, col - inside, col - inside - inside // 2)
        level = jnp.where(inner, col // cols, tail // half)
        place = jnp.where(
            inner,
            half + col % cols,
            jnp.where(low, tail % half, half + cols + tail % half),
        )
        return level, place

    def banded(place, weights):
        spot = place - lax.broadcasted_iota(jnp.int32, place.shape, 0)
        tap = weights[...].astype(F32)
        band = jnp.zeros(place.shape, F32)
        for d in range(tap.shape[1]):
            band = jnp.where(spot == d, tap[:, d : d + 1], band)
        return band

    level, place = columns(cols, rows)
    band = banded(place, static_taper)
    for q in range(levs):
        sband[q * cols : (q + 1) * cols] = jnp.where(level == q, band, 0.0).astype(BF16)
    for side_to in range(2):
        static_halo(side_to).wait_recv()
    smooth[...] = jnp.dot(sband[...], sbuf[...], preferred_element_type=F32).astype(BF16)
    zs[slot(me)] = smooth[...]

    @pl.when(gate)
    def _():
        gather_start(2)

    lanes = lpad.shape[1]
    level, place = columns(lanes, full)
    row = lax.broadcasted_iota(jnp.int32, (lanes, wide), 0)
    pick[...] = jnp.where(row == level, 1.0, 0.0).astype(BF16)
    tband[...] = banded(place[:cols], taper)

    padrows = lpad.shape[0]

    gather_far(1)
    gather_far(0)
    gather_near(1)
    gather_near(0)
    fbuf[...] = fgroup[...].astype(F32)

    def expand_loc(rank, carry):
        spread[...] = jnp.dot(lg[rank], pick[...], preferred_element_type=F32)

        def one(q, inner_carry):
            at = pl.ds(pl.multiple_of((rank * levs + q) * cols, 16), cols)
            w[at] = (spread[pl.ds(q, 1)] * tband[...]).astype(BF16)
            return inner_carry

        return lax.fori_loop(0, levs, one, carry)

    lax.fori_loop(0, nlev, expand_loc, 0)
    spread[:, :full] = jnp.dot(spad[...], pick[:, :full], preferred_element_type=F32)
    same = lax.broadcasted_iota(jnp.int32, (cols, full), 1) % cols == (
        lax.broadcasted_iota(jnp.int32, (cols, full), 0)
    )

    def expand_static(q, carry):
        at = pl.ds(pl.multiple_of(q * cols, 16), cols)
        ws[at] = jnp.where(same, spread[pl.ds(q, 1), :full], 0.0).astype(BF16)
        return carry

    lax.fori_loop(0, levs, expand_static, 0)

    nby = lats // GROUP
    nbx = cols // LINE
    levels = nlev * levs
    live = ids[...] >= 0
    local_ids = ids[...] - lon * (nbx * nby)
    by = jnp.where(live, local_ids % nby, -1)
    bx = jnp.where(live, local_ids // nby, -1)
    stage[-1].wait()
    hturn[...] = horiz[...].T

    def spread_horiz(s, carry):
        line = hturn[pl.ds(pl.multiple_of(s * GROUP, GROUP), GROUP)]
        block = jnp.concatenate([jnp.where(by == q, line, 0.0) for q in range(nby)], axis=0)
        at = pl.ds(pl.multiple_of(s * lats, lats), lats)
        hcol[at] = block.astype(BF16)
        hrow[:, at] = block.T.astype(BF16)
        return carry

    lax.fori_loop(0, LINE, spread_horiz, 0)

    gather_far(3)
    gather_near(3)
    for rank in range(nlev):
        folded = vg[rank].astype(F32)
        for p in range(folds):
            piece = folded[p * levs : (p + 1) * levs]
            lane = slice(p * 128, (p + 1) * 128)
            for q in range(nbx):
                at = slice(q * levels + rank * levs, q * levels + (rank + 1) * levs)
                vx[at, lane] = jnp.where(bx[:, lane] == q, piece, 0.0)

    own_copy.wait()

    tile = full // 3 if full % 48 == 0 else full

    steps = 2 * nlev

    def enter(e, c):
        late = e >= steps
        h = jnp.where(late, (e - steps) // 2, e // nlev)
        rank = jnp.where(late, hl - 1 + (e - steps) % 2, e % nlev)
        gated = (rank == hl - 1) | (rank == hl)
        mine = rank == me

        @pl.when(jnp.where(late, jnp.logical_not(mine), jnp.logical_not(gated) | mine))
        def _():
            @pl.when(jnp.logical_not(mine))
            def _():
                ens_copy(0, peers[0], rank, 2 * c + h).wait_recv()

            lane = pl.ds(pl.multiple_of(h * 128, 128), 128)
            product = ebuf[2 * c + h, slot(rank)].astype(F32) * fbuf[slot(rank)]
            at = pl.ds(pl.multiple_of(rank * strip, 16), strip)
            hsend[0, c, at, lane], hsend[1, c, at, lane] = edges(product)
            zbuf[c, slot(rank), lane] = product.astype(BF16)
            for side_to in range(2):
                halo_copy(side_to, c, h, rank).start()

        return c

    def chunk(c, carry):
        @pl.when(c < pairs)
        def _():
            lax.fori_loop(0, steps + 4, enter, c)

            @pl.when((c == pairs - 1) & jnp.logical_not(gate))
            def _():
                gather_start(2)

        @pl.when((c == pairs) & gate)
        def _():
            gather_far(2)

        @pl.when(c >= 1)
        def _():
            d = c - 1
            for h in range(2):
                for side_to in range(2):
                    halo_copy(side_to, d, h).wait_recv()

            def piece(q, inner_carry):
                at = pl.ds(pl.multiple_of(q * tile, 16), tile)
                zv = jnp.dot(w[at], zbuf[d], preferred_element_type=F32)
                acc[at] += (
                    ebuf[2 * d, at].astype(F32) * zv[:, :128]
                    + ebuf[2 * d + 1, at].astype(F32) * zv[:, 128:]
                )
                return inner_carry

            lax.fori_loop(0, full // tile, piece, 0)

        return carry

    lax.fori_loop(0, pairs + 1, chunk, 0)

    @pl.when(jnp.logical_not(gate))
    def _():
        gather_far(2)

    gather_near(2)
    static = jnp.dot(ws[...], zs[...], preferred_element_type=F32)
    acc[slot(me)] += (static_weight / ens_weight) * sdev[...] * static

    for q in range(nbx):
        for s in range(LINE):
            cells[q * levels : (q + 1) * levels, s * lats : (s + 1) * lats] = acc[
                pl.ds(q * LINE + s, levels, stride=cols)
            ]
    projected = jnp.dot(cells[...].astype(BF16), hcol[...], preferred_element_type=F32)
    mine = ens_weight * jnp.sum(projected * vx[...], axis=0, keepdims=True)
    part[...] = mine
    parts[me] = mine
    for off, peer in enumerate(peers):
        part_copy(off, peer, me).start()
    accb[...] = acc[...].astype(BF16)
    for off, peer in enumerate(peers):
        back_copy(off, peer).start()
    for off, rank in enumerate(sources):
        part_copy(off, peers[off], rank).wait_recv()
    hx = parts[0]
    for rank in range(1, nlev):
        hx = hx + parts[rank]
    miss = hx - value[...]
    dep = jnp.where(live, rinv[...] * miss, 0.0)
    terms = 0.5 * dep * miss
    folded = terms[:, :128]
    for q in range(1, slots // 128):
        folded = folded + terms[:, q * 128 : (q + 1) * 128]
    costs[lon] = folded
    for off in range(nlon - 1):
        cost_copy(off, lon).start()
    held = -(-levs // 8) * 8
    weighted = jnp.concatenate(
        [vert[...] * (dep / ens_weight), jnp.zeros((held - levs, slots), F32)], axis=0
    )
    chosen = jnp.concatenate([jnp.where(bx == q, weighted, 0.0) for q in range(nbx)], axis=0)
    sums = jnp.dot(chosen.astype(BF16), hrow[...], preferred_element_type=F32)
    for q in range(nbx):
        for s in range(LINE):
            both[1, pl.ds(q * LINE + s, levs, stride=cols)] = sums[
                q * held : q * held + levs, s * lats : (s + 1) * lats
            ]
    leave[1].start()
    total = acc[slot(me)]
    for off, peer in enumerate(peers):
        back_copy(off, peer).wait_recv()
        total = total + rbuf[off].astype(F32)
    both[0] = total
    leave[0].start()
    for off in range(nlon - 1):
        cost_copy(off, lax.rem(lon + nlon - off - 1, nlon)).wait_recv()
    total_cost = costs[0]
    for rank in range(1, nlon):
        total_cost = total_cost + costs[rank]
    cost[...] = jnp.sum(total_cost, axis=1, keepdims=True)

    for copy in leave:
        copy.wait()
    for off, peer in enumerate(peers):
        part_copy(off, peer, me).wait_send()
    for off in range(nlon - 1):
        cost_copy(off, lon).wait_send()
    for which in range(4):
        gather_drain(which)
    for off, peer in enumerate(peers):
        back_copy(off, peer).wait_send()
    for side_to in range(2):
        static_halo(side_to).wait_send()

    def drain(c, carry):
        for h in range(2):
            for off, peer in enumerate(peers):
                ens_copy(off, peer, me, 2 * c + h).wait_send()
            for side_to in range(2):
                halo_copy(side_to, c, h).wait_send()
        return carry

    lax.fori_loop(0, pairs, drain, 0)


def body(
    nlev,
    nlon,
    field,
    ens,
    sdev,
    lon_taper,
    static_taper,
    loc_vert,
    static_vert,
    obs_block,
    obs_value,
    obs_rinv,
    obs_horiz,
    obs_vert,
):
    members, levs, cols, lats = ens.shape
    half = lon_taper.shape[0] // 2
    pairs = members // nlev // 2
    rows = levs * cols
    full = nlev * rows
    edge = nlev * levs * half
    wide = full + 2 * edge
    slots = obs_block.shape[0]
    padrows = -(-levs // 16) * 16
    taps = lon_taper.shape[0]
    width = loc_vert.shape[1]
    picks = cols // LINE * nlev * levs
    hl = nlev // 2
    vmem = pl.BlockSpec(memory_space=pltpu.VMEM)
    dma = pltpu.SemaphoreType.DMA
    both, obs_cost = pl.pallas_call(
        functools.partial(main_kernel, (nlev, nlon, levs, cols, half, pairs)),
        out_shape=(
            jax.ShapeDtypeStruct((2, rows, lats), F32),
            jax.ShapeDtypeStruct((1, 1), F32),
        ),
        in_specs=[pl.BlockSpec(memory_space=pl.ANY)] * 12,
        out_specs=(pl.BlockSpec(memory_space=pl.ANY), vmem),
        scratch_shapes=[
            pltpu.VMEM((rows, lats), F32),
            pltpu.VMEM((rows, lats), F32),
            pltpu.VMEM((1, taps), BF16),
            pltpu.VMEM((1, taps), BF16),
            pltpu.VMEM((levs, width), BF16),
            pltpu.VMEM((levs, width), BF16),
            pltpu.VMEM((1, slots), jnp.int32),
            pltpu.VMEM((1, slots), F32),
            pltpu.VMEM((1, slots), F32),
            pltpu.VMEM((slots, lats), F32),
            pltpu.VMEM((levs, slots), F32),
            pltpu.VMEM((2 * pairs, full, lats), BF16),
            pltpu.VMEM((pairs, wide, 2 * lats), BF16),
            pltpu.VMEM((2, pairs, edge, 2 * lats), BF16),
            pltpu.VMEM((rows, lats), BF16),
            pltpu.VMEM((full, lats), BF16),
            pltpu.VMEM((full, lats), F32),
            pltpu.VMEM((rows, lats), BF16),
            pltpu.VMEM((rows, 2 * rows), BF16),
            pltpu.VMEM((2 * rows, lats), BF16),
            pltpu.VMEM((2, levs * half, lats), BF16),
            pltpu.VMEM((rows, lats), BF16),
            pltpu.VMEM((full, lats), BF16),
            pltpu.VMEM((padrows, 128), BF16),
            pltpu.VMEM((padrows, 128), BF16),
            pltpu.VMEM((nlev, padrows, 128), BF16),
            pltpu.VMEM((padrows, wide), F32),
            pltpu.VMEM((full, wide), BF16),
            pltpu.VMEM((rows, full), BF16),
            pltpu.VMEM((128, wide), BF16),
            pltpu.VMEM((cols, wide), F32),
            pltpu.VMEM((full, lats), F32),
            pltpu.VMEM((full, lats), BF16),
            pltpu.VMEM((nlev - 1, rows, lats), BF16),
            pltpu.VMEM((lats, slots), F32),
            pltpu.VMEM((LINE * lats, slots), BF16),
            pltpu.VMEM((slots, LINE * lats), BF16),
            pltpu.VMEM((picks, LINE * lats), F32),
            pltpu.VMEM((levs * slots // 128, 128), F32),
            pltpu.VMEM((levs * slots // 128, 128), BF16),
            pltpu.VMEM((nlev, levs * slots // 128, 128), BF16),
            pltpu.VMEM((picks, slots), F32),
            pltpu.VMEM((1, slots), F32),
            pltpu.VMEM((nlev, 1, slots), F32),
            pltpu.VMEM((nlon, 1, 128), F32),
            pltpu.VMEM((2, rows, lats), F32),
            dma,
            dma((2,)),
            dma((11,)),
            dma((nlev - 1, 2 * pairs)),
            dma((nlev, 2 * pairs)),
            dma((2, 2 * pairs + 1)),
            dma((2, 2 * pairs + 1)),
            dma((4, nlev - 1)),
            dma((4, nlev)),
            dma((4, hl * hl)),
            dma((nlev - 1,)),
            dma((nlev - 1,)),
            dma((nlev - 1,)),
            dma((nlev - 1,)),
            dma((nlon - 1,)),
            dma((nlon - 1,)),
        ],
        compiler_params=pltpu.CompilerParams(
            collective_id=0, has_side_effects=True, vmem_limit_bytes=63 * 1024 * 1024
        ),
        name="covariance",
    )(
        ens.reshape(members, rows, lats),
        field.reshape(rows, lats),
        sdev.reshape(rows, lats),
        lon_taper.reshape(1, -1),
        static_taper.reshape(1, -1),
        loc_vert,
        static_vert,
        obs_block.reshape(1, slots),
        obs_value.reshape(1, slots),
        obs_rinv.reshape(1, slots),
        obs_horiz,
        obs_vert.T,
    )
    shape = (levs, cols, lats)
    increment, adjoint_field = ens_weight * both[0], ens_weight * both[1]
    return (increment.reshape(shape), adjoint_field.reshape(shape), obs_cost[0, 0])


def solution(mesh):
    return jax.shard_map(
        functools.partial(body, mesh.shape["lev"], mesh.shape["lon"]),
        mesh=mesh,
        in_specs=(
            P("lev", "lon", None),
            P(None, "lev", "lon", None),
            P("lev", "lon", None),
            P(),
            P(),
            P("lev", None),
            P("lev", None),
            P("lon"),
            P("lon"),
            P("lon"),
            P("lon", None),
            P("lon", "lev"),
        ),
        out_specs=(P("lev", "lon", None), P("lev", "lon", None), P()),
        check_vma=False,
    )
```
